8 devices in a mesh: dp: 1 (over z), pp: 2 (over y), tp: 4 (over x, core).
Axes of the slice: x: 2, y: 2, z: 1, core: 2. Of those that a mesh axis runs over, the one named last changes fastest.
Arguments:
- x_in: bfloat16 [64, 64, 2048], P('dp', 'tp')
- ln_gain: bfloat16 [2, 2, 2048], P(None, 'pp')
- w_in: bfloat16 [2, 2, 2048, 8192], P(None, 'pp', None, 'tp')
- w_out: bfloat16 [2, 2, 8192, 2048], P(None, 'pp', 'tp')
Outputs:
- output: bfloat16 [64, 64, 2048], P(('dp', 'pp'), 'tp')
All inputs are finite; a program needn't handle non-finite values.
Results may differ from the reference program's by a relative error of at most 0.0176923.
Values are sent between devices in bfloat16 or wider.
A program may use at most 1 GiB of HBM per device.

```python
import jax
import jax.numpy as jnp
from jax import lax

MODEL_DIM = 2048
FFN_DIM = 8192
STAGES = 2
TP_RANKS = 4
MICRO_BATCHES = 64
SEQ_TOKENS = 64

NORM_EPS = 1e-5
SHARD_FFN = FFN_DIM // TP_RANKS
BLOCK_COUNT = 2 * STAGES


def setup_inputs(seed: int = 0, part: int = 0) -> dict:
    base_key = jax.random.key(seed)
    act_key = jax.random.fold_in(jax.random.fold_in(base_key, 1), part)
    gain_key, first_key, second_key = jax.random.split(jax.random.fold_in(base_key, 2), 3)
    x_vals = jax.random.normal(act_key, (MICRO_BATCHES, SEQ_TOKENS, MODEL_DIM), jnp.float32)
    gain_vals = 1.0 + 0.25 * jax.random.normal(gain_key, (2, STAGES, MODEL_DIM), jnp.float32)
    first_vals = jax.random.normal(first_key, (2, STAGES, MODEL_DIM, FFN_DIM), jnp.float32) * MODEL_DIM ** -0.5
    second_vals = jax.random.normal(second_key, (2, STAGES, FFN_DIM, MODEL_DIM), jnp.float32) * FFN_DIM ** -0.5
    return {"x_in": x_vals.astype(jnp.bfloat16), "ln_gain": gain_vals.astype(jnp.bfloat16), "w_in": first_vals.astype(jnp.bfloat16), "w_out": second_vals.astype(jnp.bfloat16)}


def mlp_block(resid, gain_vec, w_first, w_second):
    resid_f = resid.astype(jnp.float32)
    row_mean = jnp.mean(resid_f, axis=-1, keepdims=True)
    centred = resid_f - row_mean
    row_var = jnp.mean(centred * centred, axis=-1, keepdims=True)
    normed = (centred * lax.rsqrt(row_var + NORM_EPS) * gain_vec.astype(jnp.float32)).astype(jnp.bfloat16)
    hidden = jax.nn.gelu(jnp.dot(normed, w_first, preferred_element_type=jnp.float32)).astype(jnp.bfloat16)
    hidden_shards = hidden.reshape(SEQ_TOKENS, TP_RANKS, SHARD_FFN).transpose(1, 0, 2)
    w_shards = w_second.reshape(TP_RANKS, SHARD_FFN, MODEL_DIM)

    def add_shard(acc_sum, shard_pair):
        h_shard, w_shard = shard_pair
        part_prod = jnp.dot(h_shard, w_shard, preferred_element_type=jnp.float32)
        return acc_sum + part_prod.astype(jnp.bfloat16).astype(jnp.float32), None

    mlp_sum, _ = lax.scan(add_shard, jnp.zeros((SEQ_TOKENS, MODEL_DIM), jnp.float32), (hidden_shards, w_shards))
    return (resid_f + mlp_sum).astype(jnp.bfloat16)


def reference(x_in, ln_gain, w_in, w_out):
    gain_rows = ln_gain.reshape(BLOCK_COUNT, MODEL_DIM)
    firsts = w_in.reshape(BLOCK_COUNT, MODEL_DIM, FFN_DIM)
    seconds = w_out.reshape(BLOCK_COUNT, FFN_DIM, MODEL_DIM)

    def one_block(resid, block_w):
        gain_vec, w_first, w_second = block_w
        return mlp_block(resid, gain_vec, w_first, w_second), None

    def one_micro(micro_x):
        result, _ = lax.scan(one_block, micro_x, (gain_rows, firsts, seconds))
        return result

    return lax.map(one_micro, x_in)
```

```python
import functools

import jax
import jax.numpy as jnp
from jax import lax
from jax.experimental import pallas as pl
from jax.experimental.pallas import tpu as pltpu
from jax.sharding import PartitionSpec as P

NORM_EPS = 1e-5
MESH = pl.DeviceIdType.MESH

MICRO_PER_ITEM = 2
LOOKAHEAD = 3
LAG_FINAL = 3
COL_BLOCK = 512


def mlp_kernel(dims, x_ref, gain_ref, w1_hbm, w2_hbm, out_ref,
               w1, w2, inbox, hbuf, abuf, qbuf, pair_in, sum_out, sum_in,
               w_sem, agx_s, agx_r, agd_s, agd_r, rsd_s, rsd_r, rsx_s, rsx_r, y_s, y_r, out_r):
    items, rows, width, ring = dims
    work = 2 * items
    hid = w1.shape[2]
    stage = lax.axis_index("pp")
    rank = lax.axis_index("tp")
    cx, cc = rank // 2, rank % 2
    sibling = {"tp": 2 * cx + (1 - cc)}
    across = {"tp": 2 * (1 - cx) + cc}
    other_stage = {"pp": 1 - stage}

    @pl.when(stage == 0)
    def _():
        @pl.loop(0, items)
        def _(i):
            pltpu.make_async_copy(x_ref.at[i], inbox.at[i], y_r.at[i]).start()

    w_copies = []
    for v in range(2):
        w_copies.append((pltpu.make_async_copy(w1_hbm.at[v], w1.at[v], w_sem.at[2 * v]),
                         pltpu.make_async_copy(w2_hbm.at[v], w2.at[v], w_sem.at[2 * v + 1])))
    for pair in w_copies:
        for cp in pair:
            cp.start()

    barrier = pltpu.get_barrier_semaphore()
    for dev in (sibling, across, other_stage):
        pl.semaphore_signal(barrier, inc=1, device_id=dev, device_id_type=MESH)
    pl.semaphore_wait(barrier, 3)

    def remote(src, dst, s_sem, r_sem, dev):
        return pltpu.make_async_remote_copy(src_ref=src, dst_ref=dst, send_sem=s_sem, recv_sem=r_sem,
                                            device_id=dev, device_id_type=MESH)

    def copy_agx(slot, src_x):
        ref = hbuf.at[slot, cc, src_x]
        return remote(ref, ref, agx_s.at[slot], agx_r.at[slot], across)

    def copy_agd(slot, src_c):
        ref = hbuf.at[slot, src_c]
        return remote(ref, ref, agd_s.at[slot], agd_r.at[slot], sibling)

    def copy_rsd(slot):
        return remote(qbuf.at[slot, 1 - cc], pair_in.at[slot], rsd_s.at[slot], rsd_r.at[slot], sibling)

    def copy_rsx(slot):
        return remote(sum_out.at[slot], sum_in.at[slot], rsx_s.at[slot], rsx_r.at[slot], across)

    def norm_and_send(w):
        slot = lax.rem(w, ring)
        v = w // items
        pltpu.make_async_copy(inbox.at[w], inbox.at[w], y_r.at[w]).wait()
        y = inbox[w].astype(jnp.float32)
        mean = jnp.mean(y, axis=-1, keepdims=True)
        cen = y - mean
        var = jnp.mean(cen * cen, axis=-1, keepdims=True)
        gain = gain_ref[v].astype(jnp.float32)
        hbuf[slot, cc, cx] = (cen * lax.rsqrt(var + NORM_EPS) * gain).astype(jnp.bfloat16)
        copy_agx(slot, cx).start()

    def forward(w):
        slot = lax.rem(w, ring)
        copy_agx(slot, 1 - cx).wait_recv()
        copy_agd(slot, cc).start()

    def first_matmul(w):
        slot = lax.rem(w, ring)
        v = w // items
        copy_agd(slot, 1 - cc).wait_recv()
        for n in range(0, hid, COL_BLOCK):
            h = hbuf[slot].reshape(4 * rows, width)
            z = jnp.dot(h, w1[v, :, n:n + COL_BLOCK], preferred_element_type=jnp.float32)
            abuf[:, n:n + COL_BLOCK] = jax.nn.gelu(z).astype(jnp.bfloat16)
        copy_agx(slot, cx).wait_send()
        copy_agd(slot, cc).wait_send()

    def second_matmul(w):
        slot = lax.rem(w, ring)
        v = w // items
        for n in range(0, width, COL_BLOCK):
            q = jnp.dot(abuf[...], w2[v, :, n:n + COL_BLOCK], preferred_element_type=jnp.float32)
            qbuf[slot, :, :, :, n:n + COL_BLOCK] = q.astype(jnp.bfloat16).reshape(2, 2, rows, COL_BLOCK)
        copy_rsd(slot).start()

    def relay(w):
        slot = lax.rem(w, ring)
        cp = copy_rsd(slot)
        cp.wait_send()
        cp.wait_recv()
        total = qbuf[slot, cc, 1 - cx].astype(jnp.float32) + pair_in[slot, 1 - cx].astype(jnp.float32)
        sum_out[slot] = total.astype(jnp.bfloat16)
        copy_rsx(slot).start()

    def y_send_wait(k):
        pltpu.make_async_copy(inbox.at[0], inbox.at[0], y_s.at[k]).wait()

    def finish(w):
        slot = lax.rem(w, ring)
        v = w // items
        i = lax.rem(w, items)
        cp = copy_rsx(slot)
        cp.wait_send()
        cp.wait_recv()
        ysem = y_s.at[lax.rem(w, 2)]

        @pl.when(w >= 2)
        def _():
            y_send_wait(lax.rem(w, 2))

        total = qbuf[slot, cc, cx].astype(jnp.float32) + pair_in[slot, cx].astype(jnp.float32)
        total = total + sum_in[slot].astype(jnp.float32)
        inbox[w] = (inbox[w].astype(jnp.float32) + total).astype(jnp.bfloat16)
        last = (stage == 1) & (v == 1)
        half = items // 2

        @pl.when(jnp.logical_not(last))
        def _():
            dst = w + stage * items
            remote(inbox.at[w], inbox.at[dst], ysem, y_r.at[dst], other_stage).start()

        @pl.when(last & (i < half))
        def _():
            remote(inbox.at[w], out_ref.at[i], ysem, out_r.at[0], other_stage).start()

        @pl.when(last & (i >= half))
        def _():
            pltpu.make_async_copy(inbox.at[w], out_ref.at[i - half], ysem).start()

    for w in range(LOOKAHEAD):
        norm_and_send(w)
    forward(0)

    def tick(t, carry):
        @pl.when(t + 1 < work)
        def _():
            forward(t + 1)

        for v in range(2):
            @pl.when(t == v * items)
            def _():
                for cp in w_copies[v]:
                    cp.wait()

        @pl.when(t < work)
        def _():
            first_matmul(t)

        @pl.when((t >= 1) & (t <= work))
        def _():
            relay(t - 1)

        @pl.when(t >= LAG_FINAL)
        def _():
            finish(t - LAG_FINAL)

        @pl.when(t + LOOKAHEAD < work)
        def _():
            norm_and_send(t + LOOKAHEAD)

        @pl.when(t < work)
        def _():
            second_matmul(t)

        return carry

    lax.fori_loop(0, work + LAG_FINAL, tick, 0)
    for k in range(2):
        y_send_wait(k)

    @pl.when(stage == 0)
    def _():
        pltpu.make_async_copy(out_ref, out_ref, out_r.at[0]).wait()


def solution(mesh):
    def per_device(x_loc, gain_loc, w_in_loc, w_out_loc):
        micro, toks, width = x_loc.shape
        items = micro // MICRO_PER_ITEM
        rows = MICRO_PER_ITEM * toks
        hid = w_in_loc.shape[3]
        ring = LOOKAHEAD + LAG_FINAL
        bf16 = jnp.bfloat16
        dma = pltpu.SemaphoreType.DMA
        any_spec = pl.BlockSpec(memory_space=pl.ANY)
        flops = 2 * 2 * micro * 4 * toks * width * hid * 2
        out = pl.pallas_call(
            functools.partial(mlp_kernel, (items, rows, width, ring)),
            out_shape=jax.ShapeDtypeStruct((items // 2, rows, width), bf16),
            in_specs=[any_spec, pl.BlockSpec(memory_space=pltpu.VMEM), any_spec, any_spec],
            out_specs=any_spec,
            scratch_shapes=[
                pltpu.VMEM((2, width, hid), bf16),
                pltpu.VMEM((2, hid, width), bf16),
                pltpu.VMEM((2 * items, rows, width), bf16),
                pltpu.VMEM((ring, 2, 2, rows, width), bf16),
                pltpu.VMEM((4 * rows, hid), bf16),
                pltpu.VMEM((ring, 2, 2, rows, width), bf16),
                pltpu.VMEM((ring, 2, rows, width), bf16),
                pltpu.VMEM((ring, rows, width), bf16),
                pltpu.VMEM((ring, rows, width), bf16),
                dma((4,)),
            ] + [dma((ring,))] * 8 + [dma((2,)), dma((2 * items,)), dma((1,))],
            compiler_params=pltpu.CompilerParams(collective_id=0, has_side_effects=True,
                                                 vmem_limit_bytes=67043328),
            cost_estimate=pl.CostEstimate(flops=flops, bytes_accessed=2 ** 26, transcendentals=0),
        )(x_loc.reshape(items, rows, width), gain_loc, w_in_loc[:, 0], w_out_loc[:, 0])
        return out.reshape(micro // 2, toks, width)

    return jax.shard_map(per_device, mesh=mesh, in_specs=(P("dp", "tp", None), P(None, "pp", None), P(None, "pp", None, "tp"), P(None, "pp", "tp", None)), out_specs=P(("dp", "pp"), "tp", None), check_vma=False)
```

```python
import functools

import jax
import jax.numpy as jnp
from jax import lax
from jax.experimental import pallas as pl
from jax.experimental.pallas import tpu as pltpu
from jax.sharding import PartitionSpec as P

NORM_EPS = 1e-5
MESH = pl.DeviceIdType.MESH

MICRO_PER_ITEM = 2
LOOKAHEAD = 4
LAG_FINAL = 3
COL_BLOCK = 512
HEAD_FAR = 16
HEAD_SKIP = 3
MID_DIAG = 2
MID_FIRST = 36
LAST_DIAG = 2


def mlp_kernel(dims, x_ref, gain_ref, w1_hbm, w2_hbm, out_ref,
               w1, w2, inbox, hbuf, abuf, qbuf, pair_in, sum_out, sum_in, far,
               w_sem, agx_s, agx_r, agd_s, agd_r, rsd_s, rsd_r, rsx_s, rsx_r, y_s, y_r, out_r, far_s, far_r):
    items, rows, width, ring = dims
    work = 2 * items
    hid = w1.shape[2]
    stage = lax.axis_index("pp")
    rank = lax.axis_index("tp")
    cx, cc = rank // 2, rank % 2
    sibling = {"tp": 2 * cx + (1 - cc)}
    across = {"tp": 2 * (1 - cx) + cc}
    other_stage = {"pp": 1 - stage}
    diagonal = {"pp": 1 - stage, "tp": 2 * (1 - cx) + cc}

    def early_far(w):
        return (w < HEAD_FAR) & (lax.rem(w, HEAD_SKIP) != HEAD_SKIP - 1)

    def mid_far(w):
        return (w >= MID_FIRST) & (w < MID_FIRST + MID_DIAG)

    def last_far(w):
        return w >= work - LAST_DIAG

    def is_far(w):
        return ((stage == 0) & early_far(w)) | ((stage == 1) & (mid_far(w) | last_far(w)))

    def far_slot(w):
        late = jnp.where(w >= work - LAST_DIAG, w - (work - LAST_DIAG) + MID_DIAG, w - MID_FIRST)
        return jnp.where(w < HEAD_FAR, w, HEAD_FAR + late)

    @pl.when(stage == 0)
    def _():
        @pl.loop(0, items)
        def _(i):
            pltpu.make_async_copy(x_ref.at[i], inbox.at[i], y_r.at[i]).start()

    w_copies = []
    for v in range(2):
        w_copies.append((pltpu.make_async_copy(w1_hbm.at[v], w1.at[v], w_sem.at[2 * v]),
                         pltpu.make_async_copy(w2_hbm.at[v], w2.at[v], w_sem.at[2 * v + 1])))
    for cp in w_copies[0]:
        cp.start()

    barrier = pltpu.get_barrier_semaphore()
    for dev in (sibling, across, other_stage, diagonal):
        pl.semaphore_signal(barrier, inc=1, device_id=dev, device_id_type=MESH)
    pl.semaphore_wait(barrier, 4)

    def remote(src, dst, s_sem, r_sem, dev):
        return pltpu.make_async_remote_copy(src_ref=src, dst_ref=dst, send_sem=s_sem, recv_sem=r_sem,
                                            device_id=dev, device_id_type=MESH)

    def copy_agx(slot, src_x):
        ref = hbuf.at[slot, cc, src_x]
        return remote(ref, ref, agx_s.at[slot], agx_r.at[slot], across)

    def copy_agd(slot, src_c):
        ref = hbuf.at[slot, src_c]
        return remote(ref, ref, agd_s.at[slot], agd_r.at[slot], sibling)

    def copy_rsd(slot):
        return remote(qbuf.at[slot, 1 - cc], pair_in.at[slot], rsd_s.at[slot], rsd_r.at[slot], sibling)

    def copy_rsx(slot):
        return remote(sum_out.at[slot], sum_in.at[slot], rsx_s.at[slot], rsx_r.at[slot], across)

    def copy_far(src, k):
        return remote(src, far.at[k], far_s.at[k], far_r.at[k], diagonal)

    def head_far(k, start):
        own = k == 0

        @pl.when((stage == 0) & own)
        def _():
            cp = remote(x_ref.at[k], far.at[k], far_s.at[k], far_r.at[k], across)
            cp.start() if start else cp.wait_send()

        @pl.when((stage == 1) & jnp.logical_not(own) & early_far(k))
        def _():
            cp = copy_far(x_ref.at[k], k)
            cp.start() if start else cp.wait_send()

    @pl.loop(0, HEAD_FAR)
    def _(k):
        head_far(k, True)

    def normed(resid, v):
        y = resid.astype(jnp.float32)
        mean = jnp.mean(y, axis=-1, keepdims=True)
        cen = y - mean
        var = jnp.mean(cen * cen, axis=-1, keepdims=True)
        gain = gain_ref[v].astype(jnp.float32)
        return (cen * lax.rsqrt(var + NORM_EPS) * gain).astype(jnp.bfloat16)

    def norm_and_send(w):
        slot = lax.rem(w, ring)
        pltpu.make_async_copy(inbox.at[w], inbox.at[w], y_r.at[w]).wait()
        hbuf[slot, cc, cx] = normed(inbox[w], w // items)

        @pl.when(jnp.logical_not(is_far(w)))
        def _():
            copy_agx(slot, cx).start()

    def forward(w):
        slot = lax.rem(w, ring)

        @pl.when(jnp.logical_not(is_far(w)))
        def _():
            copy_agx(slot, 1 - cx).wait_recv()

        @pl.when(is_far(w))
        def _():
            k = far_slot(w)
            pltpu.make_async_copy(far.at[k], far.at[k], far_r.at[k]).wait()
            hbuf[slot, cc, 1 - cx] = normed(far[k], w // items)

        copy_agd(slot, cc).start()

    def first_matmul(w):
        slot = lax.rem(w, ring)
        v = w // items
        copy_agd(slot, 1 - cc).wait_recv()
        for n in range(0, hid, COL_BLOCK):
            h = hbuf[slot].reshape(4 * rows, width)
            z = jnp.dot(h, w1[v, :, n:n + COL_BLOCK], preferred_element_type=jnp.float32)
            abuf[:, n:n + COL_BLOCK] = jax.nn.gelu(z).astype(jnp.bfloat16)

        @pl.when(jnp.logical_not(is_far(w)))
        def _():
            copy_agx(slot, cx).wait_send()

        copy_agd(slot, cc).wait_send()

    def second_matmul(w):
        slot = lax.rem(w, ring)
        v = w // items
        for n in range(0, width, COL_BLOCK):
            q = jnp.dot(abuf[...], w2[v, :, n:n + COL_BLOCK], preferred_element_type=jnp.float32)
            qbuf[slot, :, :, :, n:n + COL_BLOCK] = q.astype(jnp.bfloat16).reshape(2, 2, rows, COL_BLOCK)
        copy_rsd(slot).start()

    def relay(w):
        slot = lax.rem(w, ring)
        cp = copy_rsd(slot)
        cp.wait_send()
        cp.wait_recv()
        total = qbuf[slot, cc, 1 - cx].astype(jnp.float32) + pair_in[slot, 1 - cx].astype(jnp.float32)
        sum_out[slot] = total.astype(jnp.bfloat16)
        copy_rsx(slot).start()

    def y_send_wait(k):
        pltpu.make_async_copy(inbox.at[0], inbox.at[0], y_s.at[k]).wait()

    def finish(w):
        slot = lax.rem(w, ring)
        v = w // items
        i = lax.rem(w, items)
        cp = copy_rsx(slot)
        cp.wait_send()
        cp.wait_recv()
        ysem = y_s.at[lax.rem(w, 2)]

        @pl.when(w >= 2)
        def _():
            y_send_wait(lax.rem(w, 2))

        total = qbuf[slot, cc, cx].astype(jnp.float32) + pair_in[slot, cx].astype(jnp.float32)
        total = total + sum_in[slot].astype(jnp.float32)
        inbox[w] = (inbox[w].astype(jnp.float32) + total).astype(jnp.bfloat16)
        last = (stage == 1) & (v == 1)
        half = items // 2

        @pl.when(jnp.logical_not(last))
        def _():
            dst = w + stage * items
            remote(inbox.at[w], inbox.at[dst], ysem, y_r.at[dst], other_stage).start()

        @pl.when((stage == 0) & (mid_far(w) | last_far(w)))
        def _():
            copy_far(inbox.at[w], far_slot(w)).start()

        @pl.when(last & (i < half))
        def _():
            remote(inbox.at[w], out_ref.at[i], ysem, out_r.at[0], other_stage).start()

        @pl.when(last & (i >= half))
        def _():
            pltpu.make_async_copy(inbox.at[w], out_ref.at[i - half], ysem).start()

    for w in range(LOOKAHEAD):
        norm_and_send(w)
    forward(0)

    def tick(t, carry):
        @pl.when(t + 1 < work)
        def _():
            forward(t + 1)

        @pl.when(t == 1)
        def _():
            for cp in w_copies[1]:
                cp.start()

        for v in range(2):
            @pl.when(t == v * items)
            def _():
                for cp in w_copies[v]:
                    cp.wait()

        @pl.when(t < work)
        def _():
            first_matmul(t)

        @pl.when((t >= 1) & (t <= work))
        def _():
            relay(t - 1)

        @pl.when(t >= LAG_FINAL)
        def _():
            finish(t - LAG_FINAL)

        @pl.when(t + LOOKAHEAD < work)
        def _():
            norm_and_send(t + LOOKAHEAD)

        @pl.when(t < work)
        def _():
            second_matmul(t)

        return carry

    lax.fori_loop(0, work + LAG_FINAL, tick, 0)
    for k in range(2):
        y_send_wait(k)

    @pl.loop(0, HEAD_FAR)
    def _(k):
        head_far(k, False)

    @pl.when(stage == 0)
    def _():
        for k in range(HEAD_FAR, HEAD_FAR + MID_DIAG + LAST_DIAG):
            pltpu.make_async_copy(far.at[k], far.at[k], far_s.at[k]).wait()

    @pl.when(stage == 0)
    def _():
        pltpu.make_async_copy(out_ref, out_ref, out_r.at[0]).wait()


def solution(mesh):
    def per_device(x_loc, gain_loc, w_in_loc, w_out_loc):
        micro, toks, width = x_loc.shape
        items = micro // MICRO_PER_ITEM
        rows = MICRO_PER_ITEM * toks
        hid = w_in_loc.shape[3]
        ring = LOOKAHEAD + LAG_FINAL
        bf16 = jnp.bfloat16
        dma = pltpu.SemaphoreType.DMA
        any_spec = pl.BlockSpec(memory_space=pl.ANY)
        flops = 2 * 2 * micro * 4 * toks * width * hid * 2
        out = pl.pallas_call(
            functools.partial(mlp_kernel, (items, rows, width, ring)),
            out_shape=jax.ShapeDtypeStruct((items // 2, rows, width), bf16),
            in_specs=[any_spec, pl.BlockSpec(memory_space=pltpu.VMEM), any_spec, any_spec],
            out_specs=any_spec,
            scratch_shapes=[
                pltpu.VMEM((2, width, hid), bf16),
                pltpu.VMEM((2, hid, width), bf16),
                pltpu.VMEM((2 * items, rows, width), bf16),
                pltpu.VMEM((ring, 2, 2, rows, width), bf16),
                pltpu.VMEM((4 * rows, hid), bf16),
                pltpu.VMEM((ring, 2, 2, rows, width), bf16),
                pltpu.VMEM((ring, 2, rows, width), bf16),
                pltpu.VMEM((ring, rows, width), bf16),
                pltpu.VMEM((ring, rows, width), bf16),
                pltpu.VMEM((HEAD_FAR + MID_DIAG + LAST_DIAG, rows, width), bf16),
                dma((4,)),
            ] + [dma((ring,))] * 8 + [dma((2,)), dma((2 * items,)), dma((1,))]
            + [dma((HEAD_FAR + MID_DIAG + LAST_DIAG,))] * 2,
            compiler_params=pltpu.CompilerParams(collective_id=0, has_side_effects=True,
                                                 vmem_limit_bytes=67043328),
            cost_estimate=pl.CostEstimate(flops=flops, bytes_accessed=2 ** 26, transcendentals=0),
        )(x_loc.reshape(items, rows, width), gain_loc, w_in_loc[:, 0], w_out_loc[:, 0])
        return out.reshape(micro // 2, toks, width)

    return jax.shard_map(per_device, mesh=mesh, in_specs=(P("dp", "tp", None), P(None, "pp", None), P(None, "pp", None, "tp"), P(None, "pp", "tp", None)), out_specs=P(("dp", "pp"), "tp", None), check_vma=False)
```

```python
import functools

import jax
import jax.numpy as jnp
from jax import lax
from jax.experimental import pallas as pl
from jax.experimental.pallas import tpu as pltpu
from jax.sharding import PartitionSpec as P

NORM_EPS = 1e-5
MESH = pl.DeviceIdType.MESH

MICRO_PER_ITEM = 2
LOOKAHEAD = 4
LAG_FINAL = 3
COL_BLOCK = 512
HEAD_FROM = 4
HEAD_FAR = 20
HEAD_STEP = 3
HEAD_KEEP = 1
MID_DIAG = 3
MID_FIRST = 47
MID_STEP = 4
LAST_DIAG = 2


def mlp_kernel(dims, x_ref, gain_hbm, w1_hbm, w2_hbm, out_ref,
               gains, w1, w2, inbox, hbuf, abuf, qbuf, pair_in, sum_out, sum_in, far,
               w_sem, agx_s, agx_r, agd_s, agd_r, rsd_s, rsd_r, rsx_s, rsx_r, y_s, y_r, out_r, far_s, far_r, g_sem):
    items, rows, width, ring = dims
    work = 2 * items
    half = items // 2
    hid = w1.shape[2]
    stage = lax.axis_index("pp")
    rank = lax.axis_index("tp")
    cx, cc = rank // 2, rank % 2
    sibling = {"tp": 2 * cx + (1 - cc)}
    across = {"tp": 2 * (1 - cx) + cc}
    other_stage = {"pp": 1 - stage}
    diagonal = {"pp": 1 - stage, "tp": 2 * (1 - cx) + cc}

    def early_far(w):
        return (w == 0) | ((w >= HEAD_FROM) & (w < HEAD_FAR) & (lax.rem(w, HEAD_STEP) != HEAD_KEEP))

    def mid_far(w):
        past = w - MID_FIRST
        return (past >= 0) & (past < MID_DIAG * MID_STEP) & (lax.rem(w, MID_STEP) == MID_FIRST % MID_STEP)

    def last_far(w):
        return w >= work - LAST_DIAG

    def is_far(w):
        return ((stage == 0) & early_far(w)) | ((stage == 1) & (mid_far(w) | last_far(w)))

    def far_slot(w):
        late = jnp.where(w >= work - LAST_DIAG, w - (work - LAST_DIAG) + MID_DIAG, (w - MID_FIRST) // MID_STEP)
        return jnp.where(w < HEAD_FAR, w, HEAD_FAR + late)

    gain_copy = pltpu.make_async_copy(gain_hbm, gains, g_sem.at[0])
    gain_copy.start()

    @pl.when(stage == 0)
    def _():
        @pl.loop(0, items)
        def _(i):
            pltpu.make_async_copy(x_ref.at[i], inbox.at[i], y_r.at[i]).start()

    w_copies = []
    for v in range(2):
        w_copies.append((pltpu.make_async_copy(w1_hbm.at[v], w1.at[v], w_sem.at[2 * v]),
                         pltpu.make_async_copy(w2_hbm.at[v], w2.at[v], w_sem.at[2 * v + 1])))
    for cp in w_copies[0]:
        cp.start()

    barrier = pltpu.get_barrier_semaphore()
    for dev in (sibling, across, other_stage, diagonal):
        pl.semaphore_signal(barrier, inc=1, device_id=dev, device_id_type=MESH)
    pl.semaphore_wait(barrier, 4)

    def remote(src, dst, s_sem, r_sem, dev):
        return pltpu.make_async_remote_copy(src_ref=src, dst_ref=dst, send_sem=s_sem, recv_sem=r_sem,
                                            device_id=dev, device_id_type=MESH)

    def copy_agx(slot, src_x):
        ref = hbuf.at[slot, cc, src_x]
        return remote(ref, ref, agx_s.at[slot], agx_r.at[slot], across)

    def copy_agd(slot, src_c):
        ref = hbuf.at[slot, src_c]
        return remote(ref, ref, agd_s.at[slot], agd_r.at[slot], sibling)

    def copy_rsd(slot):
        return remote(qbuf.at[slot, 1 - cc], pair_in.at[slot], rsd_s.at[slot], rsd_r.at[slot], sibling)

    def copy_rsx(slot):
        return remote(sum_out.at[slot], sum_in.at[slot], rsx_s.at[slot], rsx_r.at[slot], across)

    def copy_far(src, k):
        return remote(src, far.at[k], far_s.at[k], far_r.at[k], diagonal)

    def head_far(k, start):
        own = k == 0

        @pl.when((stage == 0) & own)
        def _():
            cp = remote(x_ref.at[k], far.at[k], far_s.at[k], far_r.at[k], across)
            cp.start() if start else cp.wait_send()

        @pl.when((stage == 1) & jnp.logical_not(own) & early_far(k))
        def _():
            cp = copy_far(x_ref.at[k], k)
            cp.start() if start else cp.wait_send()

    @pl.loop(0, HEAD_FAR)
    def _(k):
        head_far(k, True)

    def normed(resid, v):
        y = resid.astype(jnp.float32)
        mean = jnp.mean(y, axis=-1, keepdims=True)
        cen = y - mean
        var = jnp.mean(cen * cen, axis=-1, keepdims=True)
        pair = gains[...].astype(jnp.float32)
        gain = jnp.where(v == 0, pair[0:1], pair[1:2])
        return (cen * lax.rsqrt(var + NORM_EPS) * gain).astype(jnp.bfloat16)

    def norm_and_send(w):
        slot = lax.rem(w, ring)
        pltpu.make_async_copy(inbox.at[w], inbox.at[w], y_r.at[w]).wait()
        hbuf[slot, cc, cx] = normed(inbox[w], w // items)

        @pl.when(jnp.logical_not(is_far(w)))
        def _():
            copy_agx(slot, cx).start()

    def forward(w):
        slot = lax.rem(w, ring)

        @pl.when(jnp.logical_not(is_far(w)))
        def _():
            copy_agx(slot, 1 - cx).wait_recv()

        @pl.when(is_far(w))
        def _():
            k = far_slot(w)
            pltpu.make_async_copy(far.at[k], far.at[k], far_r.at[k]).wait()
            hbuf[slot, cc, 1 - cx] = normed(far[k], w // items)

        copy_agd(slot, cc).start()

    def first_matmul(w):
        slot = lax.rem(w, ring)
        v = w // items
        copy_agd(slot, 1 - cc).wait_recv()
        for n in range(0, hid, COL_BLOCK):
            h = hbuf[slot].reshape(4 * rows, width)
            z = jnp.dot(h, w1[v, :, n:n + COL_BLOCK], preferred_element_type=jnp.float32)
            abuf[:, n:n + COL_BLOCK] = jax.nn.gelu(z).astype(jnp.bfloat16)

        @pl.when(jnp.logical_not(is_far(w)))
        def _():
            copy_agx(slot, cx).wait_send()

        copy_agd(slot, cc).wait_send()

    def second_matmul(w):
        slot = lax.rem(w, ring)
        v = w // items
        for n in range(0, width, COL_BLOCK):
            q = jnp.dot(abuf[...], w2[v, :, n:n + COL_BLOCK], preferred_element_type=jnp.float32)
            qbuf[slot, :, :, :, n:n + COL_BLOCK] = q.astype(jnp.bfloat16).reshape(2, 2, rows, COL_BLOCK)
        copy_rsd(slot).start()

    def relay(w):
        slot = lax.rem(w, ring)
        cp = copy_rsd(slot)
        cp.wait_send()
        cp.wait_recv()
        total = qbuf[slot, cc, 1 - cx].astype(jnp.float32) + pair_in[slot, 1 - cx].astype(jnp.float32)
        sum_out[slot] = total.astype(jnp.bfloat16)
        copy_rsx(slot).start()

    def y_send_wait(k):
        pltpu.make_async_copy(inbox.at[0], inbox.at[0], y_s.at[k]).wait()

    def finish(w):
        slot = lax.rem(w, ring)
        v = w // items
        i = lax.rem(w, items)
        cp = copy_rsx(slot)
        cp.wait_send()
        cp.wait_recv()
        ysem = y_s.at[lax.rem(w, 2)]

        @pl.when((w >= 2) & ((stage == 0) | (w - 2 < items + half)))
        def _():
            y_send_wait(lax.rem(w, 2))

        total = qbuf[slot, cc, cx].astype(jnp.float32) + pair_in[slot, cx].astype(jnp.float32)
        total = total + sum_in[slot].astype(jnp.float32)
        new = (inbox[w].astype(jnp.float32) + total).astype(jnp.bfloat16)
        inbox[w] = new
        last = (stage == 1) & (v == 1)

        @pl.when(jnp.logical_not(last))
        def _():
            dst = w + stage * items
            remote(inbox.at[w], inbox.at[dst], ysem, y_r.at[dst], other_stage).start()

        @pl.when((stage == 0) & (mid_far(w) | last_far(w)))
        def _():
            copy_far(inbox.at[w], far_slot(w)).start()

        @pl.when(last & (i < half))
        def _():
            remote(inbox.at[w], out_ref.at[i], ysem, out_r.at[0], other_stage).start()

        @pl.when(last & (i >= half))
        def _():
            out_ref[i - half] = new

    gain_copy.wait()
    for w in range(LOOKAHEAD):
        norm_and_send(w)
    forward(0)

    def tick(t, carry):
        @pl.when(t + 1 < work)
        def _():
            forward(t + 1)

        @pl.when(t == 1)
        def _():
            for cp in w_copies[1]:
                cp.start()

        for v in range(2):
            @pl.when(t == v * items)
            def _():
                for cp in w_copies[v]:
                    cp.wait()

        @pl.when(t < work)
        def _():
            first_matmul(t)

        @pl.when((t >= 1) & (t <= work))
        def _():
            relay(t - 1)

        @pl.when(t >= LAG_FINAL)
        def _():
            finish(t - LAG_FINAL)

        @pl.when(t + LOOKAHEAD < work)
        def _():
            norm_and_send(t + LOOKAHEAD)

        @pl.when(t < work)
        def _():
            second_matmul(t)

        return carry

    lax.fori_loop(0, work + LAG_FINAL, tick, 0)
    @pl.loop(0, HEAD_FAR)
    def _(k):
        head_far(k, False)

    @pl.when(stage == 0)
    def _():
        for k in range(2):
            y_send_wait(k)
        for k in range(HEAD_FAR, HEAD_FAR + MID_DIAG + LAST_DIAG):
            pltpu.make_async_copy(far.at[k], far.at[k], far_s.at[k]).wait()

    @pl.when(stage == 0)
    def _():
        pltpu.make_async_copy(out_ref, out_ref, out_r.at[0]).wait()


def solution(mesh):
    def per_device(x_loc, gain_loc, w_in_loc, w_out_loc):
        micro, toks, width = x_loc.shape
        items = micro // MICRO_PER_ITEM
        rows = MICRO_PER_ITEM * toks
        hid = w_in_loc.shape[3]
        ring = LOOKAHEAD + LAG_FINAL
        bf16 = jnp.bfloat16
        dma = pltpu.SemaphoreType.DMA
        any_spec = pl.BlockSpec(memory_space=pl.ANY)
        flops = 2 * 2 * micro * 4 * toks * width * hid * 2
        out = pl.pallas_call(
            functools.partial(mlp_kernel, (items, rows, width, ring)),
            out_shape=pltpu.VMEM((items // 2, rows, width), bf16),
            in_specs=[any_spec] * 4,
            out_specs=pl.BlockSpec(memory_space=pltpu.VMEM),
            scratch_shapes=[
                pltpu.VMEM((2, width), bf16),
                pltpu.VMEM((2, width, hid), bf16),
                pltpu.VMEM((2, hid, width), bf16),
                pltpu.VMEM((2 * items, rows, width), bf16),
                pltpu.VMEM((ring, 2, 2, rows, width), bf16),
                pltpu.VMEM((4 * rows, hid), bf16),
                pltpu.VMEM((ring, 2, 2, rows, width), bf16),
                pltpu.VMEM((ring, 2, rows, width), bf16),
                pltpu.VMEM((ring, rows, width), bf16),
                pltpu.VMEM((ring, rows, width), bf16),
                pltpu.VMEM((HEAD_FAR + MID_DIAG + LAST_DIAG, rows, width), bf16),
                dma((4,)),
            ] + [dma((ring,))] * 8 + [dma((2,)), dma((2 * items,)), dma((1,))]
            + [dma((HEAD_FAR + MID_DIAG + LAST_DIAG,))] * 2 + [dma((1,))],
            compiler_params=pltpu.CompilerParams(collective_id=0, has_side_effects=True,
                                                 vmem_limit_bytes=60 * 2 ** 20),
            cost_estimate=pl.CostEstimate(flops=flops, bytes_accessed=2 ** 26, transcendentals=0),
        )(x_loc.reshape(items, rows, width), gain_loc[:, 0], w_in_loc[:, 0], w_out_loc[:, 0])
        return out.reshape(micro // 2, toks, width)

    return jax.shard_map(per_device, mesh=mesh, in_specs=(P("dp", "tp", None), P(None, "pp", None), P(None, "pp", None, "tp"), P(None, "pp", "tp", None)), out_specs=P(("dp", "pp"), "tp", None), check_vma=False)
```

```python
import functools

import jax
import jax.numpy as jnp
from jax import lax
from jax.experimental import pallas as pl
from jax.experimental.pallas import tpu as pltpu
from jax.sharding import PartitionSpec as P

NORM_EPS = 1e-5
MESH = pl.DeviceIdType.MESH

MICRO_PER_ITEM = 2
LOOKAHEAD = 4
TAIL_ITEMS = 2
TAIL_AHEAD = 2
LAG_FINAL = 3
COL_BLOCK = 512
HEAD_FROM = 5
HEAD_FAR = 20
HEAD_STEP = 3
HEAD_KEEP = 1
MID_DIAG = 3
MID_FIRST = 46
MID_STEP = 5
LAST_DIAG = 4


def mlp_kernel(dims, x_ref, gain_hbm, w1_hbm, w2_hbm, out_ref,
               gains, w1, w2, inbox, hbuf, abuf, qbuf, pair_in, sum_out, sum_in, far,
               w_sem, agx_s, agx_r, agd_s, agd_r, rsd_s, rsd_r, rsx_s, rsx_r, y_s, y_r, out_r, far_s, far_r, g_sem):
    items, rows, width, ring = dims
    work = 2 * items
    half = items // 2
    hid = w1.shape[2]
    stage = lax.axis_index("pp")
    rank = lax.axis_index("tp")
    cx, cc = rank // 2, rank % 2
    sibling = {"tp": 2 * cx + (1 - cc)}
    across = {"tp": 2 * (1 - cx) + cc}
    other_stage = {"pp": 1 - stage}
    diagonal = {"pp": 1 - stage, "tp": 2 * (1 - cx) + cc}

    def early_far(w):
        return (w == 0) | ((w >= HEAD_FROM) & (w < HEAD_FAR) & (lax.rem(w, HEAD_STEP) != HEAD_KEEP))

    def mid_far(w):
        past = w - MID_FIRST
        return (past >= 0) & (past < MID_DIAG * MID_STEP) & (lax.rem(w, MID_STEP) == MID_FIRST % MID_STEP)

    def last_far(w):
        return w >= work - LAST_DIAG

    def is_far(w):
        return ((stage == 0) & early_far(w)) | ((stage == 1) & (mid_far(w) | last_far(w)))

    def far_slot(w):
        late = jnp.where(w >= work - LAST_DIAG, w - (work - LAST_DIAG) + MID_DIAG, (w - MID_FIRST) // MID_STEP)
        return jnp.where(w < HEAD_FAR, w, HEAD_FAR + late)

    gain_copy = pltpu.make_async_copy(gain_hbm, gains, g_sem.at[0])
    gain_copy.start()

    @pl.when(stage == 0)
    def _():
        @pl.loop(0, items)
        def _(i):
            pltpu.make_async_copy(x_ref.at[i], inbox.at[i], y_r.at[i]).start()

    w_copies = []
    for v in range(2):
        w_copies.append((pltpu.make_async_copy(w1_hbm.at[v], w1.at[v], w_sem.at[2 * v]),
                         pltpu.make_async_copy(w2_hbm.at[v], w2.at[v], w_sem.at[2 * v + 1])))
    for cp in w_copies[0]:
        cp.start()

    barrier = pltpu.get_barrier_semaphore()
    for dev in (sibling, across, other_stage, diagonal):
        pl.semaphore_signal(barrier, inc=1, device_id=dev, device_id_type=MESH)
    pl.semaphore_wait(barrier, 4)

    def remote(src, dst, s_sem, r_sem, dev):
        return pltpu.make_async_remote_copy(src_ref=src, dst_ref=dst, send_sem=s_sem, recv_sem=r_sem,
                                            device_id=dev, device_id_type=MESH)

    def copy_agx(slot, src_x):
        ref = hbuf.at[slot, cc, src_x]
        return remote(ref, ref, agx_s.at[slot], agx_r.at[slot], across)

    def copy_agd(slot, src_c):
        ref = hbuf.at[slot, src_c]
        return remote(ref, ref, agd_s.at[slot], agd_r.at[slot], sibling)

    def copy_rsd(slot):
        return remote(qbuf.at[slot, 1 - cc], pair_in.at[slot], rsd_s.at[slot], rsd_r.at[slot], sibling)

    def copy_rsx(slot):
        return remote(sum_out.at[slot], sum_in.at[slot], rsx_s.at[slot], rsx_r.at[slot], across)

    def copy_far(src, k):
        return remote(src, far.at[k], far_s.at[k], far_r.at[k], diagonal)

    def head_far(k, start):
        own = k == 0

        @pl.when((stage == 0) & own)
        def _():
            cp = remote(x_ref.at[k], far.at[k], far_s.at[k], far_r.at[k], across)
            cp.start() if start else cp.wait_send()

        @pl.when((stage == 1) & jnp.logical_not(own) & early_far(k))
        def _():
            cp = copy_far(x_ref.at[k], k)
            cp.start() if start else cp.wait_send()

    @pl.loop(0, HEAD_FAR)
    def _(k):
        head_far(k, True)

    def normed(resid, v):
        y = resid.astype(jnp.float32)
        mean = jnp.mean(y, axis=-1, keepdims=True)
        cen = y - mean
        var = jnp.mean(cen * cen, axis=-1, keepdims=True)
        pair = gains[...].astype(jnp.float32)
        gain = jnp.where(v == 0, pair[0:1], pair[1:2])
        return (cen * lax.rsqrt(var + NORM_EPS) * gain).astype(jnp.bfloat16)

    def norm_and_send(w):
        slot = lax.rem(w, ring)
        pltpu.make_async_copy(inbox.at[w], inbox.at[w], y_r.at[w]).wait()
        hbuf[slot, cc, cx] = normed(inbox[w], w // items)

        @pl.when(jnp.logical_not(is_far(w)))
        def _():
            copy_agx(slot, cx).start()

    def forward(w):
        slot = lax.rem(w, ring)

        @pl.when(jnp.logical_not(is_far(w)))
        def _():
            copy_agx(slot, 1 - cx).wait_recv()

        @pl.when(is_far(w))
        def _():
            k = far_slot(w)
            pltpu.make_async_copy(far.at[k], far.at[k], far_r.at[k]).wait()
            hbuf[slot, cc, 1 - cx] = normed(far[k], w // items)

        copy_agd(slot, cc).start()

    def first_matmul(w):
        slot = lax.rem(w, ring)
        v = w // items
        copy_agd(slot, 1 - cc).wait_recv()
        for n in range(0, hid, COL_BLOCK):
            h = hbuf[slot].reshape(4 * rows, width)
            z = jnp.dot(h, w1[v, :, n:n + COL_BLOCK], preferred_element_type=jnp.float32)
            abuf[:, n:n + COL_BLOCK] = jax.nn.gelu(z).astype(jnp.bfloat16)

        @pl.when(jnp.logical_not(is_far(w)))
        def _():
            copy_agx(slot, cx).wait_send()

        copy_agd(slot, cc).wait_send()

    def second_matmul(w):
        slot = lax.rem(w, ring)
        v = w // items
        for n in range(0, width, COL_BLOCK):
            q = jnp.dot(abuf[...], w2[v, :, n:n + COL_BLOCK], preferred_element_type=jnp.float32)
            qbuf[slot, :, :, :, n:n + COL_BLOCK] = q.astype(jnp.bfloat16).reshape(2, 2, rows, COL_BLOCK)
        copy_rsd(slot).start()

    def relay(w):
        slot = lax.rem(w, ring)
        cp = copy_rsd(slot)
        cp.wait_send()
        cp.wait_recv()
        total = qbuf[slot, cc, 1 - cx].astype(jnp.float32) + pair_in[slot, 1 - cx].astype(jnp.float32)
        sum_out[slot] = total.astype(jnp.bfloat16)
        copy_rsx(slot).start()

    def y_send_wait(k):
        pltpu.make_async_copy(inbox.at[0], inbox.at[0], y_s.at[k]).wait()

    def finish(w):
        slot = lax.rem(w, ring)
        v = w // items
        i = lax.rem(w, items)
        cp = copy_rsx(slot)
        cp.wait_send()
        cp.wait_recv()
        ysem = y_s.at[lax.rem(w, 2)]

        @pl.when((w >= 2) & ((stage == 0) | (w - 2 < items + half)))
        def _():
            y_send_wait(lax.rem(w, 2))

        total = qbuf[slot, cc, cx].astype(jnp.float32) + pair_in[slot, cx].astype(jnp.float32)
        total = total + sum_in[slot].astype(jnp.float32)
        new = (inbox[w].astype(jnp.float32) + total).astype(jnp.bfloat16)
        inbox[w] = new
        last = (stage == 1) & (v == 1)

        @pl.when(jnp.logical_not(last))
        def _():
            dst = w + stage * items
            remote(inbox.at[w], inbox.at[dst], ysem, y_r.at[dst], other_stage).start()

        @pl.when((stage == 0) & (mid_far(w) | last_far(w)))
        def _():
            copy_far(inbox.at[w], far_slot(w)).start()

        @pl.when(last & (i < half))
        def _():
            remote(inbox.at[w], out_ref.at[i], ysem, out_r.at[0], other_stage).start()

        @pl.when(last & (i >= half))
        def _():
            out_ref[i - half] = new

    gain_copy.wait()
    for w in range(LOOKAHEAD):
        norm_and_send(w)
    forward(0)

    def tick(t, carry):
        @pl.when(t + 1 < work)
        def _():
            forward(t + 1)

        @pl.when(t == 1)
        def _():
            for cp in w_copies[1]:
                cp.start()

        for v in range(2):
            @pl.when(t == v * items)
            def _():
                for cp in w_copies[v]:
                    cp.wait()

        @pl.when(t < work)
        def _():
            first_matmul(t)

        @pl.when((t >= 1) & (t <= work))
        def _():
            relay(t - 1)

        @pl.when(t >= LAG_FINAL)
        def _():
            finish(t - LAG_FINAL)

        ahead = jnp.where((stage == 1) & (t + TAIL_AHEAD >= work - TAIL_ITEMS), TAIL_AHEAD, LOOKAHEAD)

        @pl.when((t + ahead < work) & ((ahead == TAIL_AHEAD) | (stage == 0) | (t + LOOKAHEAD < work - TAIL_ITEMS)))
        def _():
            norm_and_send(t + ahead)

        @pl.when(t < work)
        def _():
            second_matmul(t)

        return carry

    lax.fori_loop(0, work + LAG_FINAL, tick, 0)
    @pl.loop(0, HEAD_FAR)
    def _(k):
        head_far(k, False)

    @pl.when(stage == 0)
    def _():
        for k in range(2):
            y_send_wait(k)
        for k in range(HEAD_FAR, HEAD_FAR + MID_DIAG + LAST_DIAG):
            pltpu.make_async_copy(far.at[k], far.at[k], far_s.at[k]).wait()

    @pl.when(stage == 0)
    def _():
        pltpu.make_async_copy(out_ref, out_ref, out_r.at[0]).wait()


def solution(mesh):
    def per_device(x_loc, gain_loc, w_in_loc, w_out_loc):
        micro, toks, width = x_loc.shape
        items = micro // MICRO_PER_ITEM
        rows = MICRO_PER_ITEM * toks
        hid = w_in_loc.shape[3]
        ring = LOOKAHEAD + LAG_FINAL
        bf16 = jnp.bfloat16
        dma = pltpu.SemaphoreType.DMA
        any_spec = pl.BlockSpec(memory_space=pl.ANY)
        flops = 2 * 2 * micro * 4 * toks * width * hid * 2
        out = pl.pallas_call(
            functools.partial(mlp_kernel, (items, rows, width, ring)),
            out_shape=pltpu.VMEM((items // 2, rows, width), bf16),
            in_specs=[any_spec] * 4,
            out_specs=pl.BlockSpec(memory_space=pltpu.VMEM),
            scratch_shapes=[
                pltpu.VMEM((2, width), bf16),
                pltpu.VMEM((2, width, hid), bf16),
                pltpu.VMEM((2, hid, width), bf16),
                pltpu.VMEM((2 * items, rows, width), bf16),
                pltpu.VMEM((ring, 2, 2, rows, width), bf16),
                pltpu.VMEM((4 * rows, hid), bf16),
                pltpu.VMEM((ring, 2, 2, rows, width), bf16),
                pltpu.VMEM((ring, 2, rows, width), bf16),
                pltpu.VMEM((ring, rows, width), bf16),
                pltpu.VMEM((ring, rows, width), bf16),
                pltpu.VMEM((HEAD_FAR + MID_DIAG + LAST_DIAG, rows, width), bf16),
                dma((4,)),
            ] + [dma((ring,))] * 8 + [dma((2,)), dma((2 * items,)), dma((1,))]
            + [dma((HEAD_FAR + MID_DIAG + LAST_DIAG,))] * 2 + [dma((1,))],
            compiler_params=pltpu.CompilerParams(collective_id=0, has_side_effects=True,
                                                 vmem_limit_bytes=60 * 2 ** 20),
            cost_estimate=pl.CostEstimate(flops=flops, bytes_accessed=2 ** 26, transcendentals=0),
        )(x_loc.reshape(items, rows, width), gain_loc[:, 0], w_in_loc[:, 0], w_out_loc[:, 0])
        return out.reshape(micro // 2, toks, width)

    return jax.shard_map(per_device, mesh=mesh, in_specs=(P("dp", "tp", None), P(None, "pp", None), P(None, "pp", None, "tp"), P(None, "pp", "tp", None)), out_specs=P(("dp", "pp"), "tp", None), check_vma=False)
```
